256 devices in a mesh: trial: 2 (over core), bank: 4 (over x), zero: 32 (over z, y).
Axes of the slice: x: 4, y: 4, z: 8, core: 2. Of those that a mesh axis runs over, the one named last changes fastest.
Arguments:
- w_gate: float32 [128, 2048, 1024], P(('trial', 'bank'), 'zero'), parts along dimension 0, may hold values from -0.25 to 0.25
- w_up: float32 [128, 2048, 1024], P(('trial', 'bank'), 'zero'), parts along dimension 0, may hold values from -0.25 to 0.25
- router_weight: float32 [4096, 64], P(('trial', 'zero'), 'bank'), parts along dimension 0, may hold values from -0.125 to 0.125
- router_gain: float32 [4096], P(('trial', 'zero')), parts along dimension 0, may hold values from 0.25 to 1.75
Outputs:
- serve_gate: bfloat16 [128, 2048, 1024], P(('trial', 'bank'), None, 'zero'), parts along dimension 0
- serve_up: bfloat16 [128, 2048, 1024], P(('trial', 'bank'), None, 'zero'), parts along dimension 0
- scale_gate: float32 [128, 1024], P(('trial', 'bank'), 'zero'), parts along dimension 0
- scale_up: float32 [128, 1024], P(('trial', 'bank'), 'zero'), parts along dimension 0
- serve_router: bfloat16 [4096, 64], P('trial'), parts along dimension 0
The draws below stay inside these ranges and needn't reach their ends.
There are 2 independent parts, one for each index of `trial`. The reference program is written for one: setup_inputs(seed, part) draws one part's arguments, and reference() takes and returns one part's arrays. A program takes and returns all parts, laid end to end along the dimension named above; each array names one. Nothing has to cross between parts.
All inputs are finite; a program needn't handle non-finite values. Where the reference program divides by a largest or mean magnitude, that divisor is 1e-20 or more.
Results may differ from the reference program's by a relative error of at most 0.001.
Values may be sent and summed in bfloat16 or wider, within the bound.
A program may use at most 128 MiB of HBM per device.

```python
import jax
import jax.numpy as jnp

EXPERTS = 64
D_MODEL = 2048
D_EXPERT = 1024


def spiked(drawn, key, source, target, parts, factor):
    def block_of(position):
        return (jnp.arange(drawn.shape[position]) // (drawn.shape[position] // parts)).reshape((-1,) + (1,) * (drawn.ndim - 1 - position))

    near = jax.random.permutation(key, parts)[block_of(target)]
    other_side = (block_of(target) + parts // 2) % parts
    return jnp.where((block_of(source) == near) | (block_of(source) == other_side), factor * drawn, drawn)


def level_of(stream_key, dims, cuts, least, top_value):
    def one(dim, parts):
        heights = jax.random.uniform(jax.random.fold_in(jax.random.fold_in(stream_key, 6), dim), (parts,), jnp.float32, least / len(cuts), top_value / len(cuts))
        return jnp.repeat(jnp.exp(heights), dims[dim] // parts).reshape((-1,) + (1,) * (len(dims) - dim - 1))

    gain = one(*cuts[0])
    for cut in cuts[1:]:
        gain = gain * one(*cut)
    return gain


def noise(stream_key, dims, spread, bound, shards=(), held_as=jnp.bfloat16):
    gain = level_of(stream_key, dims, shards, -0.22, 0.18) if shards else 1.0
    entries = jax.random.normal(stream_key, dims, jnp.float32) * spread * gain
    return jnp.minimum(jnp.maximum(entries, -bound), bound).astype(held_as)


def noise_with(rng, extent, width, most, cuts, heavy, kind=jnp.bfloat16):
    array = width * jax.random.normal(rng, extent, jnp.float32)
    if cuts:
        array = array * level_of(rng, extent, cuts, -0.22, 0.18)
    return jnp.clip(spiked(array, jax.random.fold_in(rng, 3), *heavy), -most, most).astype(kind)


def setup_inputs(seed: int = 0, part: int = 0) -> dict:
    arg_keys = jax.random.split(jax.random.key(seed), 5)
    part_splits = jax.random.split(jax.random.fold_in(arg_keys[4], part), 5)
    return {
        "w_gate": noise_with(part_splits[0], (EXPERTS, D_MODEL, D_EXPERT), D_MODEL ** -0.5, 0.25, ((0, 4), (1, 32)), (1, 2, 32, 2.75), jnp.float32),
        "w_up": noise_with(part_splits[1], (EXPERTS, D_MODEL, D_EXPERT), D_MODEL ** -0.5, 0.25, ((0, 4), (1, 32)), (1, 2, 32, 2.75), jnp.float32),
        "router_weight": noise(part_splits[2], (D_MODEL, EXPERTS), D_MODEL ** -0.5, 0.125, ((0, 32), (1, 4)), jnp.float32),
        "router_gain": jnp.clip(1.0 + 0.15 * jax.random.normal(part_splits[3], (D_MODEL,), jnp.float32), 0.25, 1.75),
    }


def reference(w_gate, w_up, router_weight, router_gain):
    scale_gate = jnp.sum(jnp.abs(w_gate), axis=1) / D_MODEL
    serve_gate = (w_gate / jnp.expand_dims(scale_gate, 1)).astype(jnp.bfloat16)
    scale_up = jnp.sum(jnp.abs(w_up), axis=1) / D_MODEL
    serve_up = (w_up / jnp.expand_dims(scale_up, 1)).astype(jnp.bfloat16)
    serve_router = (router_weight * router_gain[:, None]).astype(jnp.bfloat16)
    return serve_gate, serve_up, scale_gate, scale_up, serve_router
```

```python
import functools

import jax
import jax.numpy as jnp
from jax import lax
from jax.experimental import pallas as pl
from jax.experimental.pallas import tpu as pltpu
from jax.sharding import PartitionSpec as P

MESH = pl.DeviceIdType.MESH
D_MODEL = 2048
PEERS = 32
BANKS = 4
MATS = 32
PAIRS = MATS // 2
COLS = 32
CHUNKS = ((0, 1), (1, 1), (2, 2), (4, 4), (8, 4), (12, 4))
LOADS = 8


def far_first(k, me):
    t, u = k // 4, lax.rem(k, 4)
    dz = 4 + (2 * lax.rem(t, 2) - 1) * ((t + 1) // 2)
    dy = 2 + (2 * lax.rem(u, 2) - 1) * ((u + 1) // 2)
    z, y = me // 4, lax.rem(me, 4)
    return lax.rem(z + dz, 8) * 4 + lax.rem(y + dy, 4)


def spread_kernel(
    gate, up, router, gain,
    rx, scales, router_out,
    w, rs_tx, rs_rx, ag_tx, ag_rx, tx, rt_tx, rt_rx,
    load_sem, rs_send, rs_recv, ag_send, ag_recv, rt_send, rt_recv, x_send, x_recv, send, recv,
):
    me, bank = lax.axis_index("zero"), lax.axis_index("bank")

    per = MATS // LOADS
    loads = []
    for n in range(LOADS):
        source = gate if n < LOADS // 2 else up
        first = n % (LOADS // 2) * per
        copy = pltpu.make_async_copy(
            source.at[pl.ds(first, per)], w.at[pl.ds(n * per, per)], load_sem.at[n]
        )
        copy.start()
        loads.append(copy)

    barrier = pltpu.get_barrier_semaphore()

    @pl.loop(0, PEERS - 1)
    def _(k):
        pl.semaphore_signal(
            barrier, inc=1, device_id={"zero": far_first(k, me)}, device_id_type=MESH
        )

    for hop in range(1, BANKS):
        pl.semaphore_signal(
            barrier, inc=1, device_id={"bank": lax.rem(bank + hop, BANKS)}, device_id_type=MESH
        )

    lane = lax.broadcasted_iota(jnp.int32, (8, 128), 1) // 32

    parts = []
    for n in range(LOADS):
        loads[n].wait()
        parts.append(jnp.sum(jnp.abs(w[n * per : (n + 1) * per]), axis=1))
    sums = jnp.concatenate(parts, axis=0)
    for q in range(8):
        blocks = [sums[8 * a : 8 * a + 8, 128 * q : 128 * q + 128] for a in range(4)]
        for r in range(4):
            tile = None
            for a in range(4):
                moved = pltpu.roll(blocks[a], (32 * (a - r)) % 128, 1) if a != r else blocks[a]
                tile = moved if tile is None else jnp.where(lane == a, moved, tile)
            rs_tx[4 * q + r] = tile

    made = router[...] * gain[...]
    rt_tx[...] = jnp.concatenate([made[:8], made[8:]], axis=1).astype(jnp.bfloat16)

    pl.semaphore_wait(barrier, PEERS - 1 + BANKS - 1)

    def to_peer(k, src, dst, send_sem, recv_sem):
        peer = far_first(k, me)
        pltpu.make_async_remote_copy(
            src_ref=src(peer), dst_ref=dst, send_sem=send_sem, recv_sem=recv_sem,
            device_id={"zero": peer}, device_id_type=MESH,
        ).start()

    def bytes_of(ref, sem):
        pltpu.make_async_copy(ref, ref, sem).wait()

    others = pl.ds(0, PEERS - 1)

    @pl.loop(0, PEERS - 1)
    def _(k):
        to_peer(k, lambda peer: rs_tx.at[peer], rs_rx.at[me], rs_send, rs_recv)

    @pl.loop(0, PEERS - 1)
    def _(k):
        to_peer(k, lambda peer: rt_tx, rt_rx.at[me], rt_send, rt_recv)

    rs_rx[me] = rs_tx[me]
    rt_rx[me] = rt_tx[...]

    bytes_of(rs_rx.at[others], rs_recv)
    scale = jnp.sum(rs_rx[...], axis=0) / D_MODEL
    scales[...] = scale
    ag_tx[...] = 1.0 / scale

    @pl.loop(0, PEERS - 1)
    def _(k):
        to_peer(k, lambda peer: ag_tx, ag_rx.at[me], ag_send, ag_recv)

    ag_rx[me] = ag_tx[...]

    bytes_of(rt_rx.at[others], rt_recv)
    for k in range(PEERS // 2):
        a, b = rt_rx[2 * k].astype(jnp.float32), rt_rx[2 * k + 1].astype(jnp.float32)
        low = jnp.concatenate([a[:, :64], b[:, :64]], axis=1)
        high = jnp.concatenate([a[:, 64:], b[:, 64:]], axis=1)
        router_out[bank, :, 128 * k : 128 * k + 128] = jnp.concatenate([low, high], axis=0).astype(
            jnp.bfloat16
        )
    crossing = []
    for hop in range(1, BANKS):
        copy = pltpu.make_async_remote_copy(
            src_ref=router_out.at[bank], dst_ref=router_out.at[bank],
            send_sem=x_send.at[hop - 1], recv_sem=x_recv.at[hop - 1],
            device_id={"bank": lax.rem(bank + hop, BANKS)}, device_id_type=MESH,
        )
        copy.start()
        crossing.append(copy)

    bytes_of(ag_rx.at[others], ag_recv)
    rows = []
    for a in range(4):
        along = []
        for q in range(8):
            block = None
            for r in range(4):
                tile = ag_rx[4 * q + r]
                moved = pltpu.roll(tile, (32 * (r - a)) % 128, 1) if a != r else tile
                block = moved if block is None else jnp.where(lane == r, moved, block)
            along.append(block)
        rows.append(along)

    for c, (first, count) in enumerate(CHUNKS):
        for p in range(first, first + count):
            for q in range(8):
                block = w[2 * p : 2 * p + 2, :, 128 * q : 128 * q + 128]
                g = 2 * p
                factor = rows[g // 8][q][g % 8 : g % 8 + 2]
                turned = (block * factor[:, None, :]).reshape(128, 128).T
                tx[4 * q : 4 * q + 4, p] = turned.astype(jnp.bfloat16).reshape(4, COLS, 128)
        span = pl.ds(first, count)

        @pl.loop(0, PEERS - 1)
        def _(k, span=span, c=c):
            to_peer(
                k, lambda peer: tx.at[peer, span], rx.at[me, span], send.at[c], recv.at[c]
            )

        rx[me, first : first + count] = tx[me, first : first + count]

    for copy in crossing:
        copy.wait()
    for c, (first, count) in enumerate(CHUNKS):
        bytes_of(rx.at[others, pl.ds(first, count)], recv.at[c])
    bytes_of(rs_rx.at[others], rs_send)
    bytes_of(rt_rx.at[others], rt_send)
    bytes_of(ag_rx.at[others], ag_send)
    for c, (first, count) in enumerate(CHUNKS):
        bytes_of(tx.at[others, pl.ds(first, count)], send.at[c])


def place_kernel(rx, scales, router_in, gate, up, scale_gate, scale_up, router, out, sem):
    whole = pltpu.make_async_copy(router_in, router, sem.at[PAIRS])
    whole.start()
    copies = []
    for p in range(PAIRS):
        for k in range(PEERS // 2):
            a, b = rx[2 * k, p].astype(jnp.float32), rx[2 * k + 1, p].astype(jnp.float32)
            here = slice(128 * k, 128 * k + 128)
            even = jnp.concatenate([a[:, :64], b[:, :64]], axis=1)
            odd = jnp.concatenate([a[:, 64:], b[:, 64:]], axis=1)
            out[2 * p, :, here] = even.astype(jnp.bfloat16)
            out[2 * p + 1, :, here] = odd.astype(jnp.bfloat16)
        target, first = (gate, 2 * p) if p < PAIRS // 2 else (up, 2 * p - MATS // 2)
        copy = pltpu.make_async_copy(
            out.at[pl.ds(2 * p, 2)], target.at[pl.ds(first, 2)], sem.at[p]
        )
        copy.start()
        copies.append(copy)
    for a in range(2):
        scale_gate[8 * a : 8 * a + 8] = scales[:, 32 * a : 32 * a + 32]
        scale_up[8 * a : 8 * a + 8] = scales[:, 64 + 32 * a : 96 + 32 * a]
    for copy in copies:
        copy.wait()
    whole.wait()


def local(w_gate, w_up, router_weight, router_gain):
    f32, bf16 = jnp.float32, jnp.bfloat16
    vmem, hbm = pl.BlockSpec(memory_space=pltpu.VMEM), pl.BlockSpec(memory_space=pltpu.HBM)
    dma = pltpu.SemaphoreType.DMA
    rx, scales, router = pl.pallas_call(
        spread_kernel,
        out_shape=(
            jax.ShapeDtypeStruct((PEERS, PAIRS, COLS, 128), bf16),
            jax.ShapeDtypeStruct((8, 128), f32),
            jax.ShapeDtypeStruct((BANKS, 16, D_MODEL), bf16),
        ),
        in_specs=[hbm, hbm, vmem, vmem],
        out_specs=(vmem, vmem, vmem),
        scratch_shapes=[
            pltpu.VMEM((MATS, 64, 1024), f32),
            pltpu.VMEM((PEERS, 8, 128), f32),
            pltpu.VMEM((PEERS, 8, 128), f32),
            pltpu.VMEM((8, 128), f32),
            pltpu.VMEM((PEERS, 8, 128), f32),
            pltpu.VMEM((PEERS, PAIRS, COLS, 128), bf16),
            pltpu.VMEM((8, 128), bf16),
            pltpu.VMEM((PEERS, 8, 128), bf16),
            dma((LOADS,)),
            *[dma(())] * 6,
            dma((BANKS - 1,)),
            dma((BANKS - 1,)),
            dma((len(CHUNKS),)),
            dma((len(CHUNKS),)),
        ],
        compiler_params=pltpu.CompilerParams(
            collective_id=0, has_side_effects=True, vmem_limit_bytes=46 * 2**20
        ),
    )(w_gate, w_up, router_weight.T, router_gain.reshape(1, -1))
    serve_gate, serve_up, scale_gate, scale_up, router = pl.pallas_call(
        place_kernel,
        out_shape=(
            jax.ShapeDtypeStruct((16, COLS, D_MODEL), bf16),
            jax.ShapeDtypeStruct((16, COLS, D_MODEL), bf16),
            jax.ShapeDtypeStruct((16, COLS), f32),
            jax.ShapeDtypeStruct((16, COLS), f32),
            jax.ShapeDtypeStruct((BANKS, 16, D_MODEL), bf16),
        ),
        in_specs=[vmem, vmem, vmem],
        out_specs=(hbm, hbm, vmem, vmem, hbm),
        scratch_shapes=[pltpu.VMEM((MATS, COLS, D_MODEL), bf16), dma((PAIRS + 1,))],
        compiler_params=pltpu.CompilerParams(vmem_limit_bytes=32 * 2**20),
    )(rx, scales, router)
    return (
        jnp.swapaxes(serve_gate, 1, 2),
        jnp.swapaxes(serve_up, 1, 2),
        scale_gate,
        scale_up,
        router.reshape(BANKS * 16, D_MODEL).T,
    )


def solution(mesh):
    placed = (
        P(("trial", "bank"), "zero", None),
        P(("trial", "bank"), "zero", None),
        P(("trial", "zero"), "bank"),
        P(("trial", "zero")),
    )
    return jax.shard_map(
        local,
        mesh=mesh,
        in_specs=placed,
        out_specs=(
            P(("trial", "bank"), None, "zero"),
            P(("trial", "bank"), None, "zero"),
            P(("trial", "bank"), "zero"),
            P(("trial", "bank"), "zero"),
            P("trial", None),
        ),
        check_vma=False,
    )
```

```python
import jax
import jax.numpy as jnp
from jax import lax
from jax.experimental import pallas as pl
from jax.experimental.pallas import tpu as pltpu
from jax.sharding import PartitionSpec as P

MESH = pl.DeviceIdType.MESH
D_MODEL = 2048
PEERS = 32
BANKS = 4
MATS = 32
BLOCKS = ((0, 0), (1, 0), (0, 4), (0, 8), (0, 12), (1, 4), (1, 8), (1, 12))
PAIRS = MATS // 2
COLS = 32
CHUNKS = ((0, 1), (1, 1), (2, 2), (4, 1), (5, 1), (6, 2), (8, 4), (12, 3), (15, 1))
CODED = 4
POWER = 13
TOP = 2.0**9
LEAST = 1e-30
LOADS = 8


def far_first(k, me):
    t, u = k // 4, lax.rem(k, 4)
    dz = 4 + (2 * lax.rem(t, 2) - 1) * ((t + 1) // 2)
    dy = 2 + (2 * lax.rem(u, 2) - 1) * ((u + 1) // 2)
    z, y = me // 4, lax.rem(me, 4)
    return lax.rem(z + dz, 8) * 4 + lax.rem(y + dy, 4)


def joined(left, right):
    left, right = left.astype(jnp.float32), right.astype(jnp.float32)
    return (
        jnp.concatenate([left[:, :64], right[:, :64]], axis=1),
        jnp.concatenate([left[:, 64:], right[:, 64:]], axis=1),
    )


def tile_of(block, factor):
    return (block * factor[:, None, :]).reshape(128, 128)


def decoded(tile, factor):
    v = tile.astype(jnp.float32)
    size = jnp.exp(jnp.log(jnp.abs(v)) * (1.0 / POWER)) * factor
    return jnp.where(v == 0.0, 0.0, jnp.where(v < 0.0, -size, size))


def spread_kernel(
    gate, up, router, gain,
    placed, scale_gate, scale_up, router_out,
    w, rs_tx, rs_rx, ag_tx, ag_z, ag_y, turned, tx, rx, rt_in, gain_in, rt_tx, rt_z, rt_y,
    load_sem, rs_send, rs_recv, az_send, az_recv, ay_send, ay_recv,
    z_send, z_recv, y_send, y_recv,
    x_send, x_recv, send, recv,
):
    me, bank = lax.axis_index("zero"), lax.axis_index("bank")
    z, y = me // 4, lax.rem(me, 4)

    per = MATS // LOADS
    loads = []
    for n, (which, first) in enumerate(BLOCKS):
        copy = pltpu.make_async_copy(
            (gate, up)[which].at[pl.ds(first, per)], w.at[pl.ds(n * per, per)], load_sem.at[n]
        )
        copy.start()
        loads.append(copy)

    small = []
    for n, (source, target) in enumerate(((router, rt_in), (gain, gain_in))):
        copy = pltpu.make_async_copy(source, target, load_sem.at[LOADS + n])
        copy.start()
        small.append(copy)

    barrier = pltpu.get_barrier_semaphore()

    @pl.loop(0, PEERS - 1)
    def _(k):
        pl.semaphore_signal(
            barrier, inc=1, device_id={"zero": far_first(k, me)}, device_id_type=MESH
        )

    for hop in range(1, BANKS):
        pl.semaphore_signal(
            barrier, inc=1, device_id={"bank": lax.rem(bank + hop, BANKS)}, device_id_type=MESH
        )

    lane = lax.broadcasted_iota(jnp.int32, (8, 128), 1) // 32

    def encode(p, sums):
        own = TOP / jnp.maximum(sums, LEAST)
        for q in range(8):
            here = slice(128 * q, 128 * q + 128)
            x = tile_of(w[2 * p : 2 * p + 2, :, here], own[:, here])
            x2 = x * x
            x4 = x2 * x2
            x12 = (x4 * x4) * x4
            tx[4 * q : 4 * q + 4, p] = (x12 * x).T.astype(jnp.bfloat16).reshape(4, COLS, 128)

    def sums_of(n):
        loads[n].wait()
        return jnp.sum(jnp.abs(w[n * per : (n + 1) * per]), axis=1)

    def to_zero(peer, src, dst, send_sem, recv_sem):
        pltpu.make_async_remote_copy(
            src_ref=src, dst_ref=dst, send_sem=send_sem, recv_sem=recv_sem,
            device_id={"zero": peer}, device_id_type=MESH,
        ).start()

    def to_peer(k, src, dst, send_sem, recv_sem):
        peer = far_first(k, me)
        to_zero(peer, src(peer), dst, send_sem, recv_sem)

    def bytes_of(ref, sem):
        pltpu.make_async_copy(ref, ref, sem).wait()

    others = pl.ds(0, PEERS - 1)

    def send_chunk(c):
        first, count = CHUNKS[c]
        span = pl.ds(first, count)

        @pl.loop(0, PEERS - 1)
        def _(k):
            to_peer(
                k, lambda peer: tx.at[peer, span], rx.at[me, span], send.at[c], recv.at[c]
            )

        rx[me, first : first + count] = tx[me, first : first + count]

    parts = [sums_of(0)]
    encode(0, parts[0][:2])
    pl.semaphore_wait(barrier, PEERS - 1 + BANKS - 1)
    send_chunk(0)

    for n in range(1, LOADS):
        parts.append(sums_of(n))
    sums = jnp.concatenate(parts, axis=0)
    for q in range(8):
        blocks = [sums[8 * a : 8 * a + 8, 128 * q : 128 * q + 128] for a in range(4)]
        for r in range(4):
            tile = None
            for a in range(4):
                moved = pltpu.roll(blocks[a], (32 * (a - r)) % 128, 1) if a != r else blocks[a]
                tile = moved if tile is None else jnp.where(lane == a, moved, tile)
            rs_tx[4 * q + r] = tile

    @pl.loop(0, PEERS - 1)
    def _(k):
        to_peer(k, lambda peer: rs_tx.at[peer], rs_rx.at[me], rs_send, rs_recv)

    encode(1, parts[0][2:])
    send_chunk(1)

    for copy in small:
        copy.wait()
    made = rt_in[...] * gain_in[...]
    rt_tx[...] = jnp.concatenate([made[:8], made[8:]], axis=1).astype(jnp.bfloat16)

    for hop in (4, 3, 5, 2, 6, 1, 7):
        to_zero(lax.rem(z + hop, 8) * 4 + y, rt_tx, rt_z.at[z], z_send, z_recv)

    rs_rx[me] = rs_tx[me]
    rt_z[z] = rt_tx[...]
    for p in range(2, CODED):
        encode(p, parts[1][2 * p - 4 : 2 * p - 2])

    bytes_of(rs_rx.at[others], rs_recv)
    scale = jnp.sum(rs_rx[...], axis=0) / D_MODEL
    for n, (which, first) in enumerate(BLOCKS):
        target = (scale_gate, scale_up)[which]
        target[first : first + per] = scale[
            n * per % 8 : n * per % 8 + per, n // 2 * COLS : n // 2 * COLS + COLS
        ]
    ag_tx[...] = 1.0 / scale

    for hop in (4, 3, 5, 2, 6, 1, 7):
        to_zero(lax.rem(z + hop, 8) * 4 + y, ag_tx, ag_z.at[z], az_send, az_recv)
    ag_z[z] = ag_tx[...]

    send_chunk(2)

    bytes_of(rt_z.at[pl.ds(0, 7)], z_recv)
    for hop in (2, 1, 3):
        to_zero(z * 4 + lax.rem(y + hop, 4), rt_z, rt_y.at[y], y_send, y_recv)
    rt_y[y] = rt_z[...]

    bytes_of(ag_z.at[pl.ds(0, 7)], az_recv)
    for hop in (2, 1, 3):
        to_zero(z * 4 + lax.rem(y + hop, 4), ag_z, ag_y.at[y], ay_send, ay_recv)
    ag_y[y] = ag_z[...]

    back = (1.0 / TOP) / scale
    for k in range(PEERS):
        turned[k] = (jnp.maximum(rs_rx[k], LEAST) * back).T[:COLS]

    bytes_of(ag_y.at[pl.ds(0, 3)], ay_recv)
    rows = []
    for a in range(1, 4):
        along = []
        for q in range(8):
            block = None
            for r in range(4):
                tile = ag_y[r, q]
                moved = pltpu.roll(tile, (32 * (r - a)) % 128, 1) if a != r else tile
                block = moved if block is None else jnp.where(lane == r, moved, block)
            along.append(block)
        rows.append(along)

    for c in range(3, len(CHUNKS)):
        first, count = CHUNKS[c]
        for p in range(first, first + count):
            for q in range(8):
                g = 2 * p
                x = tile_of(
                    w[g : g + 2, :, 128 * q : 128 * q + 128], rows[g // 8 - 1][q][g % 8 : g % 8 + 2]
                )
                tx[4 * q : 4 * q + 4, p] = x.T.astype(jnp.bfloat16).reshape(4, COLS, 128)
        send_chunk(c)

    bytes_of(rt_y.at[pl.ds(0, 3)], y_recv)
    for k in range(PEERS // 2):
        low, high = joined(rt_y[2 * (k % 2), k // 2], rt_y[2 * (k % 2) + 1, k // 2])
        router_out[bank, :, 128 * k : 128 * k + 128] = jnp.concatenate([low, high], axis=0).astype(
            jnp.bfloat16
        )
    crossing = []
    half = lax.broadcasted_iota(jnp.int32, (COLS, 128), 1) < 64
    for hop in range(1, BANKS):
        copy = pltpu.make_async_remote_copy(
            src_ref=router_out.at[bank], dst_ref=router_out.at[bank],
            send_sem=x_send.at[hop - 1], recv_sem=x_recv.at[hop - 1],
            device_id={"bank": lax.rem(bank + hop, BANKS)}, device_id_type=MESH,
        )
        copy.start()
        crossing.append(copy)

    for c, (first, count) in enumerate(CHUNKS):
        bytes_of(rx.at[others, pl.ds(first, count)], recv.at[c])
        for p in range(first, first + count):
            for k in range(PEERS // 2):
                pair = []
                for n in (2 * k, 2 * k + 1):
                    tile = rx[n, p]
                    if p < CODED:
                        both = turned[n]
                        factor = jnp.where(
                            half, both[:, 2 * p : 2 * p + 1], both[:, 2 * p + 1 : 2 * p + 2]
                        )
                        tile = decoded(tile, factor)
                    pair.append(tile)
                even, odd = joined(*pair)
                here = slice(128 * k, 128 * k + 128)
                placed[2 * p, :, here] = even.astype(jnp.bfloat16)
                placed[2 * p + 1, :, here] = odd.astype(jnp.bfloat16)

    for copy in crossing:
        copy.wait()
    bytes_of(rs_rx.at[others], rs_send)
    bytes_of(ag_z.at[pl.ds(0, 7)], az_send)
    bytes_of(ag_y.at[pl.ds(0, 3)], ay_send)
    bytes_of(rt_z.at[pl.ds(0, 7)], z_send)
    bytes_of(rt_y.at[pl.ds(0, 3)], y_send)
    for c, (first, count) in enumerate(CHUNKS):
        bytes_of(tx.at[others, pl.ds(first, count)], send.at[c])


def store_kernel(placed, scale_gate, scale_up, router, *out):
    gate_out, up_out, scale_gate_out, scale_up_out, router_out, sem = out
    per = MATS // LOADS
    moves = [(scale_gate, scale_gate_out), (scale_up, scale_up_out)]
    for n, (which, first) in enumerate(BLOCKS):
        target = (gate_out, up_out)[which]
        moves.append((placed.at[pl.ds(n * per, per)], target.at[pl.ds(first, per)]))
    moves.append((router, router_out))
    copies = [pltpu.make_async_copy(a, b, sem.at[n]) for n, (a, b) in enumerate(moves)]
    for copy in copies:
        copy.start()
    for copy in copies:
        copy.wait()


def local(w_gate, w_up, router_weight, router_gain):
    f32, bf16 = jnp.float32, jnp.bfloat16
    vmem, anywhere = pl.BlockSpec(memory_space=pltpu.VMEM), pl.BlockSpec(memory_space=pl.ANY)
    dma = pltpu.SemaphoreType.DMA
    given = (w_gate, w_up, router_weight.T, router_gain.reshape(1, -1))
    served = jax.ShapeDtypeStruct((16, COLS, D_MODEL), bf16)
    scale = jax.ShapeDtypeStruct((16, COLS), f32)
    router = jax.ShapeDtypeStruct((BANKS, 16, D_MODEL), bf16)
    arrived = pl.pallas_call(
        spread_kernel,
        out_shape=(jax.ShapeDtypeStruct((MATS, COLS, D_MODEL), bf16), scale, scale, router),
        in_specs=[anywhere] * 4,
        out_specs=(vmem,) * 4,
        scratch_shapes=[
            pltpu.VMEM((MATS, 64, 1024), f32),
            pltpu.VMEM((PEERS, 8, 128), f32),
            pltpu.VMEM((PEERS, 8, 128), f32),
            pltpu.VMEM((8, 128), f32),
            pltpu.VMEM((8, 8, 128), f32),
            pltpu.VMEM((4, 8, 8, 128), f32),
            pltpu.VMEM((PEERS, COLS, 8), f32),
            pltpu.VMEM((PEERS, PAIRS, COLS, 128), bf16),
            pltpu.VMEM((PEERS, PAIRS, COLS, 128), bf16),
            pltpu.VMEM((16, 64), f32),
            pltpu.VMEM((1, 64), f32),
            pltpu.VMEM((8, 128), bf16),
            pltpu.VMEM((8, 8, 128), bf16),
            pltpu.VMEM((4, 8, 8, 128), bf16),
            dma((LOADS + 2,)),
            *[dma(())] * 10,
            dma((BANKS - 1,)),
            dma((BANKS - 1,)),
            dma((len(CHUNKS),)),
            dma((len(CHUNKS),)),
        ],
        compiler_params=pltpu.CompilerParams(
            collective_id=0, has_side_effects=True, vmem_limit_bytes=46 * 2**20
        ),
    )(*[pltpu.with_memory_space_constraint(a, pltpu.HBM) for a in given])
    serve_gate, serve_up, scale_gate, scale_up, router = pl.pallas_call(
        store_kernel,
        out_shape=(served, served, scale, scale, router),
        in_specs=[vmem] * 4,
        out_specs=(anywhere,) * 5,
        scratch_shapes=[dma((11,))],
        compiler_params=pltpu.CompilerParams(vmem_limit_bytes=32 * 2**20),
    )(*arrived)
    return (
        jnp.swapaxes(serve_gate, 1, 2),
        jnp.swapaxes(serve_up, 1, 2),
        scale_gate,
        scale_up,
        router.reshape(BANKS * 16, D_MODEL).T,
    )


def solution(mesh):
    placed = (
        P(("trial", "bank"), "zero", None),
        P(("trial", "bank"), "zero", None),
        P(("trial", "zero"), "bank"),
        P(("trial", "zero")),
    )
    return jax.shard_map(
        local,
        mesh=mesh,
        in_specs=placed,
        out_specs=(
            P(("trial", "bank"), None, "zero"),
            P(("trial", "bank"), None, "zero"),
            P(("trial", "bank"), "zero"),
            P(("trial", "bank"), "zero"),
            P("trial", None),
        ),
        check_vma=False,
    )
```

```python
import jax
import jax.numpy as jnp
from jax import lax
from jax.experimental import pallas as pl
from jax.experimental.pallas import tpu as pltpu
from jax.sharding import PartitionSpec as P

MESH = pl.DeviceIdType.MESH
D_MODEL = 2048
PEERS = 32
BANKS = 4
MATS = 32
PAIRS = MATS // 2
COLS = 32
BLOCKS = ((0, 0), (1, 0), (0, 2), (1, 2), (0, 4)) + tuple(
    [(0, e) for e in range(6, 16, 2)] + [(1, e) for e in range(4, 16, 2)]
)
CHUNKS = ((0, 1), (1, 1), (2, 1), (3, 1), (4, 1), (5, 1), (6, 2), (8, 4), (12, 3), (15, 1))
CODED = 5
POWER = 13
TOP = 2.0**9
LEAST = 1e-30
Z_HOPS, Y_HOPS = (4, 3, 5, 2, 6, 1, 7), (2, 1, 3)


def far_first(k, me):
    t, u = k // 4, lax.rem(k, 4)
    dz = 4 + (2 * lax.rem(t, 2) - 1) * ((t + 1) // 2)
    dy = 2 + (2 * lax.rem(u, 2) - 1) * ((u + 1) // 2)
    z, y = me // 4, lax.rem(me, 4)
    return lax.rem(z + dz, 8) * 4 + lax.rem(y + dy, 4)


def joined(left, right):
    left, right = left.astype(jnp.float32), right.astype(jnp.float32)
    return (
        jnp.concatenate([left[:, :64], right[:, :64]], axis=1),
        jnp.concatenate([left[:, 64:], right[:, 64:]], axis=1),
    )


def tile_of(block, factor):
    return (block * factor[:, None, :]).reshape(128, 128)


def decoded(tile, factor):
    v = tile.astype(jnp.float32)
    size = jnp.exp(jnp.log(jnp.abs(v)) * (1.0 / POWER)) * factor
    return jnp.where(v == 0.0, 0.0, jnp.where(v < 0.0, -size, size))


def spread_kernel(
    gate, up, router, gain,
    placed, scale_gate, scale_up, router_out,
    w, rs_tx, rs_y, rs_zt, rs_z, nm_tx, nm_z, nm_y, nm_t, ag_tx, ag_z, ag_y, turned, tx, rx,
    rt_in, gain_in, rt_tx, rt_z, rt_y,
    load_sem, stage_send, stage_recv, x_send, x_recv, send, recv,
):
    me, bank = lax.axis_index("zero"), lax.axis_index("bank")
    z, y = me // 4, lax.rem(me, 4)

    loads = []
    for n, (which, first) in enumerate(BLOCKS):
        copy = pltpu.make_async_copy(
            (gate, up)[which].at[pl.ds(first, 2)], w.at[pl.ds(2 * n, 2)], load_sem.at[n]
        )
        copy.start()
        loads.append(copy)
    small = []
    for n, (source, target) in enumerate(((router, rt_in), (gain, gain_in))):
        copy = pltpu.make_async_copy(source, target, load_sem.at[PAIRS + n])
        copy.start()
        small.append(copy)

    barrier = pltpu.get_barrier_semaphore()

    @pl.loop(0, PEERS - 1)
    def _(k):
        pl.semaphore_signal(
            barrier, inc=1, device_id={"zero": far_first(k, me)}, device_id_type=MESH
        )

    for hop in range(1, BANKS):
        pl.semaphore_signal(
            barrier, inc=1, device_id={"bank": lax.rem(bank + hop, BANKS)}, device_id_type=MESH
        )

    lane = lax.broadcasted_iota(jnp.int32, (8, 128), 1) // 32

    def encode(p):
        norm = jnp.maximum(norms[p].astype(jnp.float32), LEAST)
        own = TOP / norm
        for q in range(8):
            here = slice(128 * q, 128 * q + 128)
            x = tile_of(w[2 * p : 2 * p + 2, :, here], own[:, here])
            x2 = x * x
            x4 = x2 * x2
            x12 = (x4 * x4) * x4
            tx[4 * q : 4 * q + 4, p] = (x12 * x).T.astype(jnp.bfloat16).reshape(4, COLS, 128)

    def sums_of(n):
        loads[n].wait()
        return jnp.sum(jnp.abs(w[2 * n : 2 * n + 2]), axis=1)

    def to_zero(peer, src, dst, send_sem, recv_sem):
        pltpu.make_async_remote_copy(
            src_ref=src, dst_ref=dst, send_sem=send_sem, recv_sem=recv_sem,
            device_id={"zero": peer}, device_id_type=MESH,
        ).start()

    def to_peer(k, src, dst, send_sem, recv_sem):
        peer = far_first(k, me)
        to_zero(peer, src(peer), dst, send_sem, recv_sem)

    def bytes_of(ref, sem):
        pltpu.make_async_copy(ref, ref, sem).wait()

    others = pl.ds(0, PEERS - 1)

    def along_z(n, src, dst):
        for hop in Z_HOPS:
            there = lax.rem(z + hop, 8)
            to_zero(there * 4 + y, src(there), dst.at[z], stage_send.at[n], stage_recv.at[n])

    def along_y(n, src, dst):
        for hop in Y_HOPS:
            there = lax.rem(y + hop, 4)
            to_zero(z * 4 + there, src(there), dst.at[y], stage_send.at[n], stage_recv.at[n])

    def arrived_z(n, dst):
        bytes_of(dst.at[pl.ds(0, 7)], stage_recv.at[n])

    def arrived_y(n, dst):
        bytes_of(dst.at[pl.ds(0, 3)], stage_recv.at[n])

    def send_chunk(c):
        first, count = CHUNKS[c]
        span = pl.ds(first, count)

        @pl.loop(0, PEERS - 1)
        def _(k):
            to_peer(
                k, lambda peer: tx.at[peer, span], rx.at[me, span], send.at[c], recv.at[c]
            )

        rx[me, first : first + count] = tx[me, first : first + count]

    parts = [sums_of(0)]
    norms = [parts[0].astype(jnp.bfloat16)]
    encode(0)
    pl.semaphore_wait(barrier, PEERS - 1 + BANKS - 1)
    send_chunk(0)

    for n in range(1, PAIRS):
        parts.append(sums_of(n))
    norms += [parts[n].astype(jnp.bfloat16) for n in range(1, CODED)]
    sums = jnp.concatenate(parts, axis=0)
    for q in range(8):
        blocks = [sums[8 * a : 8 * a + 8, 128 * q : 128 * q + 128] for a in range(4)]
        nm_tx[q] = jnp.concatenate(blocks[:2], axis=0).astype(jnp.bfloat16)
        for r in range(4):
            tile = None
            for a in range(4):
                moved = pltpu.roll(blocks[a], (32 * (a - r)) % 128, 1) if a != r else blocks[a]
                tile = moved if tile is None else jnp.where(lane == a, moved, tile)
            rs_tx[r, q] = tile
    along_y(0, lambda there: rs_tx.at[there], rs_y)
    rs_y[y] = rs_tx[y]

    encode(1)
    send_chunk(1)

    for copy in small:
        copy.wait()
    made = rt_in[...] * gain_in[...]
    rt_tx[...] = jnp.concatenate([made[:8], made[8:]], axis=1).astype(jnp.bfloat16)
    along_z(1, lambda there: nm_tx.at[there], nm_z)
    along_z(2, lambda there: rt_tx, rt_z)
    nm_z[z] = nm_tx[z]
    rt_z[z] = rt_tx[...]
    encode(2)

    arrived_y(0, rs_y)
    rs_zt[...] = jnp.sum(rs_y[...], axis=0)
    along_z(3, lambda there: rs_zt.at[there], rs_z)
    rs_z[z] = rs_zt[z]
    send_chunk(2)
    encode(3)

    arrived_z(3, rs_z)
    scale = jnp.sum(rs_z[...], axis=0) / D_MODEL
    ag_tx[...] = 1.0 / scale
    along_z(4, lambda there: ag_tx, ag_z)
    ag_z[z] = ag_tx[...]
    send_chunk(3)
    encode(4)

    for n, (which, first) in enumerate(BLOCKS):
        target = (scale_gate, scale_up)[which]
        target[first : first + 2] = scale[
            2 * n % 8 : 2 * n % 8 + 2, n // 4 * COLS : n // 4 * COLS + COLS
        ]
    arrived_z(1, nm_z)
    along_y(5, lambda there: nm_z, nm_y)
    nm_y[y] = nm_z[...]
    arrived_z(2, rt_z)
    along_y(6, lambda there: rt_z, rt_y)
    rt_y[y] = rt_z[...]

    arrived_z(4, ag_z)
    along_y(7, lambda there: ag_z, ag_y)
    ag_y[y] = ag_z[...]
    send_chunk(4)

    arrived_y(7, ag_y)
    rows = []
    for a in range(CODED // 4, 4):
        along = []
        for q in range(8):
            block = None
            for r in range(4):
                tile = ag_y[r, q]
                moved = pltpu.roll(tile, (32 * (r - a)) % 128, 1) if a != r else tile
                block = moved if block is None else jnp.where(lane == r, moved, block)
            along.append(block)
        rows.append(along)

    for c in range(CODED, len(CHUNKS)):
        first, count = CHUNKS[c]
        for p in range(first, first + count):
            for q in range(8):
                g = 2 * p
                x = tile_of(
                    w[g : g + 2, :, 128 * q : 128 * q + 128],
                    rows[g // 8 - CODED // 4][q][g % 8 : g % 8 + 2],
                )
                tx[4 * q : 4 * q + 4, p] = x.T.astype(jnp.bfloat16).reshape(4, COLS, 128)
        send_chunk(c)

    back = ((1.0 / TOP) / scale).T
    back = jnp.concatenate([back[:COLS], back[COLS : 2 * COLS]], axis=1)
    arrived_y(5, nm_y)
    for k in range(PEERS):
        nm_t[k] = jnp.maximum(nm_y[k % 4, k // 4].astype(jnp.float32), LEAST).T
    mine = pl.ds(pl.multiple_of(COLS * y, COLS), COLS)
    for k in range(PEERS):
        turned[k] = nm_t[k, mine] * back

    arrived_y(6, rt_y)
    for k in range(PEERS // 2):
        low, high = joined(rt_y[2 * (k % 2), k // 2], rt_y[2 * (k % 2) + 1, k // 2])
        router_out[bank, :, 128 * k : 128 * k + 128] = jnp.concatenate([low, high], axis=0).astype(
            jnp.bfloat16
        )
    crossing = []
    half = lax.broadcasted_iota(jnp.int32, (COLS, 128), 1) < 64
    for hop in range(1, BANKS):
        copy = pltpu.make_async_remote_copy(
            src_ref=router_out.at[bank], dst_ref=router_out.at[bank],
            send_sem=x_send.at[hop - 1], recv_sem=x_recv.at[hop - 1],
            device_id={"bank": lax.rem(bank + hop, BANKS)}, device_id_type=MESH,
        )
        copy.start()
        crossing.append(copy)

    for c, (first, count) in enumerate(CHUNKS):
        bytes_of(rx.at[others, pl.ds(first, count)], recv.at[c])
        for p in range(first, first + count):
            for k in range(PEERS // 2):
                pair = []
                for n in (2 * k, 2 * k + 1):
                    tile = rx[n, p]
                    if p < CODED:
                        both = turned[n]
                        factor = jnp.where(
                            half, both[:, 2 * p : 2 * p + 1], both[:, 2 * p + 1 : 2 * p + 2]
                        )
                        tile = decoded(tile, factor)
                    pair.append(tile)
                even, odd = joined(*pair)
                here = slice(128 * k, 128 * k + 128)
                placed[2 * p, :, here] = even.astype(jnp.bfloat16)
                placed[2 * p + 1, :, here] = odd.astype(jnp.bfloat16)

    for copy in crossing:
        copy.wait()
    for n, sent in enumerate((rs_y, nm_z, rt_z, rs_z, ag_z, nm_y, rt_y, ag_y)):
        bytes_of(sent.at[pl.ds(0, sent.shape[0] - 1)], stage_send.at[n])
    for c, (first, count) in enumerate(CHUNKS):
        bytes_of(tx.at[others, pl.ds(first, count)], send.at[c])


def store_kernel(placed, scale_gate, scale_up, router, *out):
    gate_out, up_out, scale_gate_out, scale_up_out, router_out, sem = out
    moves = [(scale_gate, scale_gate_out), (scale_up, scale_up_out)]
    runs = []
    for n, (which, first) in enumerate(BLOCKS):
        if runs and runs[-1][0] == which and runs[-1][1] + runs[-1][3] == first:
            runs[-1][3] += 2
        else:
            runs.append([which, first, 2 * n, 2])
    for which, first, at, count in runs:
        target = (gate_out, up_out)[which]
        moves.append((placed.at[pl.ds(at, count)], target.at[pl.ds(first, count)]))
    moves.append((router, router_out))
    copies = [pltpu.make_async_copy(a, b, sem.at[n]) for n, (a, b) in enumerate(moves)]
    for copy in copies:
        copy.start()
    for copy in copies:
        copy.wait()


def local(w_gate, w_up, router_weight, router_gain):
    f32, bf16 = jnp.float32, jnp.bfloat16
    vmem, anywhere = pl.BlockSpec(memory_space=pltpu.VMEM), pl.BlockSpec(memory_space=pl.ANY)
    dma = pltpu.SemaphoreType.DMA
    given = (w_gate, w_up, router_weight.T, router_gain.reshape(1, -1))
    served = jax.ShapeDtypeStruct((16, COLS, D_MODEL), bf16)
    scale = jax.ShapeDtypeStruct((16, COLS), f32)
    router = jax.ShapeDtypeStruct((BANKS, 16, D_MODEL), bf16)
    arrived = pl.pallas_call(
        spread_kernel,
        out_shape=(jax.ShapeDtypeStruct((MATS, COLS, D_MODEL), bf16), scale, scale, router),
        in_specs=[anywhere] * 4,
        out_specs=(vmem,) * 4,
        scratch_shapes=[
            pltpu.VMEM((MATS, 64, 1024), f32),
            pltpu.VMEM((4, 8, 8, 128), f32),
            pltpu.VMEM((4, 8, 8, 128), f32),
            pltpu.VMEM((8, 8, 128), f32),
            pltpu.VMEM((8, 8, 128), f32),
            pltpu.VMEM((8, 16, 128), bf16),
            pltpu.VMEM((8, 16, 128), bf16),
            pltpu.VMEM((4, 8, 16, 128), bf16),
            pltpu.VMEM((PEERS, 128, 16), f32),
            pltpu.VMEM((8, 128), f32),
            pltpu.VMEM((8, 8, 128), f32),
            pltpu.VMEM((4, 8, 8, 128), f32),
            pltpu.VMEM((PEERS, COLS, 16), f32),
            pltpu.VMEM((PEERS, PAIRS, COLS, 128), bf16),
            pltpu.VMEM((PEERS, PAIRS, COLS, 128), bf16),
            pltpu.VMEM((16, 64), f32),
            pltpu.VMEM((1, 64), f32),
            pltpu.VMEM((8, 128), bf16),
            pltpu.VMEM((8, 8, 128), bf16),
            pltpu.VMEM((4, 8, 8, 128), bf16),
            dma((PAIRS + 2,)),
            dma((8,)),
            dma((8,)),
            dma((BANKS - 1,)),
            dma((BANKS - 1,)),
            dma((len(CHUNKS),)),
            dma((len(CHUNKS),)),
        ],
        compiler_params=pltpu.CompilerParams(
            collective_id=0, has_side_effects=True, vmem_limit_bytes=46 * 2**20
        ),
    )(*[pltpu.with_memory_space_constraint(a, pltpu.HBM) for a in given])
    serve_gate, serve_up, scale_gate, scale_up, router = pl.pallas_call(
        store_kernel,
        out_shape=(served, served, scale, scale, router),
        in_specs=[vmem] * 4,
        out_specs=(anywhere,) * 5,
        scratch_shapes=[dma((16,))],
        compiler_params=pltpu.CompilerParams(vmem_limit_bytes=32 * 2**20),
    )(*arrived)
    return (
        jnp.swapaxes(serve_gate, 1, 2),
        jnp.swapaxes(serve_up, 1, 2),
        scale_gate,
        scale_up,
        router.reshape(BANKS * 16, D_MODEL).T,
    )


def solution(mesh):
    placed = (
        P(("trial", "bank"), "zero", None),
        P(("trial", "bank"), "zero", None),
        P(("trial", "zero"), "bank"),
        P(("trial", "zero")),
    )
    return jax.shard_map(
        local,
        mesh=mesh,
        in_specs=placed,
        out_specs=(
            P(("trial", "bank"), None, "zero"),
            P(("trial", "bank"), None, "zero"),
            P(("trial", "bank"), "zero"),
            P(("trial", "bank"), "zero"),
            P("trial", None),
        ),
        check_vma=False,
    )
```

```python
import jax
import jax.numpy as jnp
from jax import lax
from jax.experimental import pallas as pl
from jax.experimental.pallas import tpu as pltpu
from jax.sharding import PartitionSpec as P

MESH = pl.DeviceIdType.MESH
D_MODEL = 2048
PEERS = 32
BANKS = 4
MATS = 32
PAIRS = MATS // 2
COLS = 32
BLOCKS = ((0, 0), (1, 0), (0, 2), (1, 2), (0, 4)) + tuple(
    [(0, e) for e in range(6, 16, 2)] + [(1, e) for e in range(4, 16, 2)]
)
CHUNKS = ((0, 1), (1, 1), (2, 1), (3, 1), (4, 1), (5, 1), (6, 2), (8, 3), (11, 3), (14, 1), (15, 1))
CODED = 5
POWER = 13
TOP = 2.0**9
LEAST = 1e-30
Z_HOPS, Y_HOPS = (4, 3, 5, 2, 6, 1, 7), (2, 1, 3)


HOPS = sorted(
    ((dz, dy) for dz in range(8) for dy in range(4) if (dz, dy) != (0, 0)),
    key=lambda hop: (-min(hop[0], 8 - hop[0]) - min(hop[1], 4 - hop[1]), hop),
)


def far_first(k, me):
    dz, dy = HOPS[k]
    return lax.rem(me // 4 + dz, 8) * 4 + lax.rem(lax.rem(me, 4) + dy, 4)


def joined(left, right):
    left, right = left.astype(jnp.float32), right.astype(jnp.float32)
    return (
        jnp.concatenate([left[:, :64], right[:, :64]], axis=1),
        jnp.concatenate([left[:, 64:], right[:, 64:]], axis=1),
    )


def tile_of(block, factor):
    return (block * factor[:, None, :]).reshape(128, 128)


def decoded(tile, factor):
    v = tile.astype(jnp.float32)
    size = jnp.exp(jnp.log(jnp.abs(v)) * (1.0 / POWER)) * factor
    return jnp.where(v == 0.0, 0.0, jnp.where(v < 0.0, -size, size))


def spread_kernel(
    gate, up, router, gain,
    placed, scale_gate, scale_up, router_out,
    w, rs_tx, rs_y, rs_zt, rs_z, nm_tx, nm_z, nm_y, nm_t, ag_tx, ag_z, ag_y, turned, tx, rx,
    rt_in, gain_in, rt_tx, rt_z, rt_y,
    load_sem, stage_send, stage_recv, x_send, x_recv, send, recv,
):
    me, bank = lax.axis_index("zero"), lax.axis_index("bank")
    z, y = me // 4, lax.rem(me, 4)

    loads = []
    for n, (which, first) in enumerate(BLOCKS):
        copy = pltpu.make_async_copy(
            (gate, up)[which].at[pl.ds(first, 2)], w.at[pl.ds(2 * n, 2)], load_sem.at[n]
        )
        copy.start()
        loads.append(copy)
    small = []
    for n, (source, target) in enumerate(((router, rt_in), (gain, gain_in))):
        copy = pltpu.make_async_copy(source, target, load_sem.at[PAIRS + n])
        copy.start()
        small.append(copy)

    barrier = pltpu.get_barrier_semaphore()

    for k in range(PEERS - 1):
        pl.semaphore_signal(
            barrier, inc=1, device_id={"zero": far_first(k, me)}, device_id_type=MESH
        )

    for hop in range(1, BANKS):
        pl.semaphore_signal(
            barrier, inc=1, device_id={"bank": lax.rem(bank + hop, BANKS)}, device_id_type=MESH
        )

    lane = lax.broadcasted_iota(jnp.int32, (8, 128), 1) // 32

    def encode(p):
        norm = jnp.maximum(norms[p].astype(jnp.float32), LEAST)
        own = TOP / norm
        for q in range(8):
            here = slice(128 * q, 128 * q + 128)
            x = tile_of(w[2 * p : 2 * p + 2, :, here], own[:, here])
            x2 = x * x
            x4 = x2 * x2
            x12 = (x4 * x4) * x4
            tx[4 * q : 4 * q + 4, p] = (x12 * x).T.astype(jnp.bfloat16).reshape(4, COLS, 128)

    def sums_of(n):
        loads[n].wait()
        return jnp.sum(jnp.abs(w[2 * n : 2 * n + 2]), axis=1)

    def to_zero(peer, src, dst, send_sem, recv_sem):
        pltpu.make_async_remote_copy(
            src_ref=src, dst_ref=dst, send_sem=send_sem, recv_sem=recv_sem,
            device_id={"zero": peer}, device_id_type=MESH,
        ).start()

    def to_peer(k, src, dst, send_sem, recv_sem):
        peer = far_first(k, me)
        to_zero(peer, src(peer), dst, send_sem, recv_sem)

    def bytes_of(ref, sem):
        pltpu.make_async_copy(ref, ref, sem).wait()

    others = pl.ds(0, PEERS - 1)

    def along_z(n, src, dst):
        for hop in Z_HOPS:
            there = lax.rem(z + hop, 8)
            to_zero(there * 4 + y, src(there), dst.at[z], stage_send.at[n], stage_recv.at[n])

    def along_y(n, src, dst):
        for hop in Y_HOPS:
            there = lax.rem(y + hop, 4)
            to_zero(z * 4 + there, src(there), dst.at[y], stage_send.at[n], stage_recv.at[n])

    def arrived_z(n, dst):
        bytes_of(dst.at[pl.ds(0, 7)], stage_recv.at[n])

    def arrived_y(n, dst):
        bytes_of(dst.at[pl.ds(0, 3)], stage_recv.at[n])

    def send_chunk(c):
        first, count = CHUNKS[c]
        span = pl.ds(first, count)

        for k in range(PEERS - 1):
            to_peer(
                k, lambda peer: tx.at[peer, span], rx.at[me, span], send.at[c], recv.at[c]
            )

        rx[me, first : first + count] = tx[me, first : first + count]

    parts = [sums_of(0)]
    norms = [parts[0].astype(jnp.bfloat16)]
    encode(0)
    pl.semaphore_wait(barrier, PEERS - 1 + BANKS - 1)
    send_chunk(0)

    for n in range(1, PAIRS):
        parts.append(sums_of(n))
    norms += [parts[n].astype(jnp.bfloat16) for n in range(1, CODED)]
    sums = jnp.concatenate(parts, axis=0)
    for q in range(8):
        blocks = [sums[8 * a : 8 * a + 8, 128 * q : 128 * q + 128] for a in range(4)]
        nm_tx[q] = jnp.concatenate(blocks[:2], axis=0).astype(jnp.bfloat16)
        for r in range(4):
            tile = None
            for a in range(4):
                moved = pltpu.roll(blocks[a], (32 * (a - r)) % 128, 1) if a != r else blocks[a]
                tile = moved if tile is None else jnp.where(lane == a, moved, tile)
            rs_tx[r, q] = tile
    along_y(0, lambda there: rs_tx.at[there], rs_y)
    rs_y[y] = rs_tx[y]

    encode(1)
    send_chunk(1)

    for copy in small:
        copy.wait()
    made = rt_in[...] * gain_in[...]
    rt_tx[...] = jnp.concatenate([made[:8], made[8:]], axis=1).astype(jnp.bfloat16)
    along_z(1, lambda there: nm_tx.at[there], nm_z)
    along_z(2, lambda there: rt_tx, rt_z)
    nm_z[z] = nm_tx[z]
    rt_z[z] = rt_tx[...]
    encode(2)

    arrived_y(0, rs_y)
    rs_zt[...] = jnp.sum(rs_y[...], axis=0)
    along_z(3, lambda there: rs_zt.at[there], rs_z)
    rs_z[z] = rs_zt[z]
    send_chunk(2)
    encode(3)

    arrived_z(3, rs_z)
    scale = jnp.sum(rs_z[...], axis=0) / D_MODEL
    ag_tx[...] = 1.0 / scale
    along_z(4, lambda there: ag_tx, ag_z)
    ag_z[z] = ag_tx[...]
    send_chunk(3)
    encode(4)

    for n, (which, first) in enumerate(BLOCKS):
        target = (scale_gate, scale_up)[which]
        target[first : first + 2] = scale[
            2 * n % 8 : 2 * n % 8 + 2, n // 4 * COLS : n // 4 * COLS + COLS
        ]
    arrived_z(1, nm_z)
    along_y(5, lambda there: nm_z, nm_y)
    nm_y[y] = nm_z[...]
    arrived_z(2, rt_z)
    along_y(6, lambda there: rt_z, rt_y)
    rt_y[y] = rt_z[...]

    arrived_z(4, ag_z)
    along_y(7, lambda there: ag_z, ag_y)
    ag_y[y] = ag_z[...]
    send_chunk(4)

    arrived_y(7, ag_y)
    rows = []
    for a in range(CODED // 4, 4):
        along = []
        for q in range(8):
            block = None
            for r in range(4):
                tile = ag_y[r, q]
                moved = pltpu.roll(tile, (32 * (r - a)) % 128, 1) if a != r else tile
                block = moved if block is None else jnp.where(lane == r, moved, block)
            along.append(block)
        rows.append(along)

    for c in range(CODED, len(CHUNKS)):
        first, count = CHUNKS[c]
        for p in range(first, first + count):
            for q in range(8):
                g = 2 * p
                x = tile_of(
                    w[g : g + 2, :, 128 * q : 128 * q + 128],
                    rows[g // 8 - CODED // 4][q][g % 8 : g % 8 + 2],
                )
                tx[4 * q : 4 * q + 4, p] = x.T.astype(jnp.bfloat16).reshape(4, COLS, 128)
        send_chunk(c)

    back = ((1.0 / TOP) / scale).T
    back = jnp.concatenate([back[:COLS], back[COLS : 2 * COLS]], axis=1)
    arrived_y(5, nm_y)
    for k in range(PEERS):
        nm_t[k] = jnp.maximum(nm_y[k % 4, k // 4].astype(jnp.float32), LEAST).T
    mine = pl.ds(pl.multiple_of(COLS * y, COLS), COLS)
    for k in range(PEERS):
        turned[k] = nm_t[k, mine] * back

    arrived_y(6, rt_y)
    for k in range(PEERS // 2):
        low, high = joined(rt_y[2 * (k % 2), k // 2], rt_y[2 * (k % 2) + 1, k // 2])
        router_out[bank, :, 128 * k : 128 * k + 128] = jnp.concatenate([low, high], axis=0).astype(
            jnp.bfloat16
        )
    crossing = []
    half = lax.broadcasted_iota(jnp.int32, (COLS, 128), 1) < 64
    for hop in range(1, BANKS):
        copy = pltpu.make_async_remote_copy(
            src_ref=router_out.at[bank], dst_ref=router_out.at[bank],
            send_sem=x_send.at[hop - 1], recv_sem=x_recv.at[hop - 1],
            device_id={"bank": lax.rem(bank + hop, BANKS)}, device_id_type=MESH,
        )
        copy.start()
        crossing.append(copy)

    for c, (first, count) in enumerate(CHUNKS):
        bytes_of(rx.at[others, pl.ds(first, count)], recv.at[c])
        for p in range(first, first + count):
            for k in range(PEERS // 2):
                pair = []
                for n in (2 * k, 2 * k + 1):
                    tile = rx[n, p]
                    if p < CODED:
                        both = turned[n]
                        factor = jnp.where(
                            half, both[:, 2 * p : 2 * p + 1], both[:, 2 * p + 1 : 2 * p + 2]
                        )
                        tile = decoded(tile, factor)
                    pair.append(tile)
                even, odd = joined(*pair)
                here = slice(128 * k, 128 * k + 128)
                placed[2 * p, :, here] = even.astype(jnp.bfloat16)
                placed[2 * p + 1, :, here] = odd.astype(jnp.bfloat16)

    for copy in crossing:
        copy.wait()
    for n, sent in enumerate((rs_y, nm_z, rt_z, rs_z, ag_z, nm_y, rt_y, ag_y)):
        bytes_of(sent.at[pl.ds(0, sent.shape[0] - 1)], stage_send.at[n])
    for c, (first, count) in enumerate(CHUNKS):
        bytes_of(tx.at[others, pl.ds(first, count)], send.at[c])


def store_kernel(placed, scale_gate, scale_up, router, *out):
    gate_out, up_out, scale_gate_out, scale_up_out, router_out, sem = out
    moves = [(scale_gate, scale_gate_out), (scale_up, scale_up_out)]
    runs = []
    for n, (which, first) in enumerate(BLOCKS):
        if runs and runs[-1][0] == which and runs[-1][1] + runs[-1][3] == first:
            runs[-1][3] += 2
        else:
            runs.append([which, first, 2 * n, 2])
    for which, first, at, count in runs:
        target = (gate_out, up_out)[which]
        moves.append((placed.at[pl.ds(at, count)], target.at[pl.ds(first, count)]))
    moves.append((router, router_out))
    copies = [pltpu.make_async_copy(a, b, sem.at[n]) for n, (a, b) in enumerate(moves)]
    for copy in copies:
        copy.start()
    for copy in copies:
        copy.wait()


def local(w_gate, w_up, router_weight, router_gain):
    f32, bf16 = jnp.float32, jnp.bfloat16
    vmem, anywhere = pl.BlockSpec(memory_space=pltpu.VMEM), pl.BlockSpec(memory_space=pl.ANY)
    dma = pltpu.SemaphoreType.DMA
    given = (w_gate, w_up, router_weight.T, router_gain.reshape(1, -1))
    served = jax.ShapeDtypeStruct((16, COLS, D_MODEL), bf16)
    scale = jax.ShapeDtypeStruct((16, COLS), f32)
    router = jax.ShapeDtypeStruct((BANKS, 16, D_MODEL), bf16)
    arrived = pl.pallas_call(
        spread_kernel,
        out_shape=(jax.ShapeDtypeStruct((MATS, COLS, D_MODEL), bf16), scale, scale, router),
        in_specs=[anywhere] * 4,
        out_specs=(vmem,) * 4,
        scratch_shapes=[
            pltpu.VMEM((MATS, 64, 1024), f32),
            pltpu.VMEM((4, 8, 8, 128), f32),
            pltpu.VMEM((4, 8, 8, 128), f32),
            pltpu.VMEM((8, 8, 128), f32),
            pltpu.VMEM((8, 8, 128), f32),
            pltpu.VMEM((8, 16, 128), bf16),
            pltpu.VMEM((8, 16, 128), bf16),
            pltpu.VMEM((4, 8, 16, 128), bf16),
            pltpu.VMEM((PEERS, 128, 16), f32),
            pltpu.VMEM((8, 128), f32),
            pltpu.VMEM((8, 8, 128), f32),
            pltpu.VMEM((4, 8, 8, 128), f32),
            pltpu.VMEM((PEERS, COLS, 16), f32),
            pltpu.VMEM((PEERS, PAIRS, COLS, 128), bf16),
            pltpu.VMEM((PEERS, PAIRS, COLS, 128), bf16),
            pltpu.VMEM((16, 64), f32),
            pltpu.VMEM((1, 64), f32),
            pltpu.VMEM((8, 128), bf16),
            pltpu.VMEM((8, 8, 128), bf16),
            pltpu.VMEM((4, 8, 8, 128), bf16),
            dma((PAIRS + 2,)),
            dma((8,)),
            dma((8,)),
            dma((BANKS - 1,)),
            dma((BANKS - 1,)),
            dma((len(CHUNKS),)),
            dma((len(CHUNKS),)),
        ],
        compiler_params=pltpu.CompilerParams(
            collective_id=0, has_side_effects=True, vmem_limit_bytes=46 * 2**20
        ),
    )(*[pltpu.with_memory_space_constraint(a, pltpu.HBM) for a in given])
    serve_gate, serve_up, scale_gate, scale_up, router = pl.pallas_call(
        store_kernel,
        out_shape=(served, served, scale, scale, router),
        in_specs=[vmem] * 4,
        out_specs=(anywhere,) * 5,
        scratch_shapes=[dma((16,))],
        compiler_params=pltpu.CompilerParams(vmem_limit_bytes=32 * 2**20),
    )(*arrived)
    return (
        jnp.swapaxes(serve_gate, 1, 2),
        jnp.swapaxes(serve_up, 1, 2),
        scale_gate,
        scale_up,
        router.reshape(BANKS * 16, D_MODEL).T,
    )


def solution(mesh):
    placed = (
        P(("trial", "bank"), "zero", None),
        P(("trial", "bank"), "zero", None),
        P(("trial", "zero"), "bank"),
        P(("trial", "zero")),
    )
    return jax.shard_map(
        local,
        mesh=mesh,
        in_specs=placed,
        out_specs=(
            P(("trial", "bank"), None, "zero"),
            P(("trial", "bank"), None, "zero"),
            P(("trial", "bank"), "zero"),
            P(("trial", "bank"), "zero"),
            P("trial", None),
        ),
        check_vma=False,
    )
```

```python
import jax
import jax.numpy as jnp
from jax import lax
from jax.experimental import pallas as pl
from jax.experimental.pallas import tpu as pltpu
from jax.sharding import PartitionSpec as P

MESH = pl.DeviceIdType.MESH
D_MODEL = 2048
PEERS = 32
BANKS = 4
MATS = 32
PAIRS = MATS // 2
COLS = 32
BLOCKS = ((0, 0), (1, 0), (0, 2), (1, 2), (0, 4)) + tuple(
    [(0, e) for e in range(6, 16, 2)] + [(1, e) for e in range(4, 16, 2)]
)
CHUNKS = ((0, 1), (1, 1), (2, 1), (3, 1), (4, 1), (5, 1), (6, 2), (8, 3), (11, 3), (14, 1), (15, 1))
CODED = 5
POWER = 13
TOP = 2.0**9
LEAST = 1e-30
Z_HOPS, Y_HOPS = (4, 3, 5, 2, 6, 1, 7), (2, 1, 3)


HOPS = sorted(
    ((dz, dy) for dz in range(8) for dy in range(4) if (dz, dy) != (0, 0)),
    key=lambda hop: (-min(hop[0], 8 - hop[0]) - min(hop[1], 4 - hop[1]), hop),
)


def far_first(k, me):
    dz, dy = HOPS[k]
    return lax.rem(me // 4 + dz, 8) * 4 + lax.rem(lax.rem(me, 4) + dy, 4)


def joined(left, right):
    left, right = left.astype(jnp.float32), right.astype(jnp.float32)
    return (
        jnp.concatenate([left[:, :64], right[:, :64]], axis=1),
        jnp.concatenate([left[:, 64:], right[:, 64:]], axis=1),
    )


def tile_of(block, factor):
    return (block * factor[:, None, :]).reshape(128, 128)


def decoded(tile, factor):
    v = tile.astype(jnp.float32)
    size = jnp.exp(jnp.log(jnp.abs(v)) * (1.0 / POWER)) * factor
    return jnp.where(v == 0.0, 0.0, jnp.where(v < 0.0, -size, size))


def spread_kernel(
    gate, up, router, gain,
    placed, scale_gate, scale_up, router_out,
    w, rs_tx, rs_y, rs_zt, rs_z, nm_tx, nm_z, nm_y, nm_t, ag_tx, ag_z, ag_y, turned, tx, rx,
    rt_in, gain_in, rt_tx, rt_z, rt_y,
    load_sem, stage_send, stage_recv, x_send, x_recv, send, recv,
):
    me, bank = lax.axis_index("zero"), lax.axis_index("bank")
    z, y = me // 4, lax.rem(me, 4)

    barrier = pltpu.get_barrier_semaphore()

    for k in range(PEERS - 1):
        pl.semaphore_signal(
            barrier, inc=1, device_id={"zero": far_first(k, me)}, device_id_type=MESH
        )

    for hop in range(1, BANKS):
        pl.semaphore_signal(
            barrier, inc=1, device_id={"bank": lax.rem(bank + hop, BANKS)}, device_id_type=MESH
        )


    loads = []
    for n, (which, first) in enumerate(BLOCKS):
        copy = pltpu.make_async_copy(
            (gate, up)[which].at[pl.ds(first, 2)], w.at[pl.ds(2 * n, 2)], load_sem.at[n]
        )
        copy.start()
        loads.append(copy)
    small = []
    for n, (source, target) in enumerate(((router, rt_in), (gain, gain_in))):
        copy = pltpu.make_async_copy(source, target, load_sem.at[PAIRS + n])
        copy.start()
        small.append(copy)

    lane = lax.broadcasted_iota(jnp.int32, (8, 128), 1) // 32

    def encode(p):
        norm = jnp.maximum(norms[p].astype(jnp.float32), LEAST)
        own = TOP / norm
        for q in range(8):
            here = slice(128 * q, 128 * q + 128)
            x = tile_of(w[2 * p : 2 * p + 2, :, here], own[:, here])
            x2 = x * x
            x4 = x2 * x2
            x12 = (x4 * x4) * x4
            tx[4 * q : 4 * q + 4, p] = (x12 * x).T.astype(jnp.bfloat16).reshape(4, COLS, 128)

    def sums_of(n):
        loads[n].wait()
        return jnp.sum(jnp.abs(w[2 * n : 2 * n + 2]), axis=1)

    def to_zero(peer, src, dst, send_sem, recv_sem):
        pltpu.make_async_remote_copy(
            src_ref=src, dst_ref=dst, send_sem=send_sem, recv_sem=recv_sem,
            device_id={"zero": peer}, device_id_type=MESH,
        ).start()

    def to_peer(k, src, dst, send_sem, recv_sem):
        peer = far_first(k, me)
        to_zero(peer, src(peer), dst, send_sem, recv_sem)

    def bytes_of(ref, sem):
        pltpu.make_async_copy(ref, ref, sem).wait()

    others = pl.ds(0, PEERS - 1)

    def along_z(n, src, dst):
        for hop in Z_HOPS:
            there = lax.rem(z + hop, 8)
            to_zero(there * 4 + y, src(there), dst.at[z], stage_send.at[n], stage_recv.at[n])

    def along_y(n, src, dst):
        for hop in Y_HOPS:
            there = lax.rem(y + hop, 4)
            to_zero(z * 4 + there, src(there), dst.at[y], stage_send.at[n], stage_recv.at[n])

    def arrived_z(n, dst):
        bytes_of(dst.at[pl.ds(0, 7)], stage_recv.at[n])

    def arrived_y(n, dst):
        bytes_of(dst.at[pl.ds(0, 3)], stage_recv.at[n])

    def send_chunk(c):
        first, count = CHUNKS[c]
        span = pl.ds(first, count)

        for k in range(PEERS - 1):
            to_peer(
                k, lambda peer: tx.at[peer, span], rx.at[me, span], send.at[c], recv.at[c]
            )

        rx[me, first : first + count] = tx[me, first : first + count]

    parts = [sums_of(0)]
    norms = [parts[0].astype(jnp.bfloat16)]
    encode(0)
    pl.semaphore_wait(barrier, PEERS - 1 + BANKS - 1)
    send_chunk(0)

    for n in range(1, PAIRS):
        parts.append(sums_of(n))
    norms += [parts[n].astype(jnp.bfloat16) for n in range(1, CODED)]
    sums = jnp.concatenate(parts, axis=0)
    for q in range(8):
        blocks = [sums[8 * a : 8 * a + 8, 128 * q : 128 * q + 128] for a in range(4)]
        nm_tx[q] = jnp.concatenate(blocks[:2], axis=0).astype(jnp.bfloat16)
        for r in range(4):
            tile = None
            for a in range(4):
                moved = pltpu.roll(blocks[a], (32 * (a - r)) % 128, 1) if a != r else blocks[a]
                tile = moved if tile is None else jnp.where(lane == a, moved, tile)
            rs_tx[r, q] = tile
    along_y(0, lambda there: rs_tx.at[there], rs_y)
    rs_y[y] = rs_tx[y]

    encode(1)
    send_chunk(1)

    for copy in small:
        copy.wait()
    made = rt_in[...] * gain_in[...]
    rt_tx[...] = jnp.concatenate([made[:8], made[8:]], axis=1).astype(jnp.bfloat16)
    along_z(1, lambda there: nm_tx.at[there], nm_z)
    along_z(2, lambda there: rt_tx, rt_z)
    nm_z[z] = nm_tx[z]
    rt_z[z] = rt_tx[...]
    encode(2)

    arrived_y(0, rs_y)
    rs_zt[...] = jnp.sum(rs_y[...], axis=0)
    along_z(3, lambda there: rs_zt.at[there], rs_z)
    rs_z[z] = rs_zt[z]
    send_chunk(2)
    encode(3)

    arrived_z(3, rs_z)
    scale = jnp.sum(rs_z[...], axis=0) / D_MODEL
    ag_tx[...] = 1.0 / scale
    along_z(4, lambda there: ag_tx, ag_z)
    ag_z[z] = ag_tx[...]
    send_chunk(3)
    encode(4)

    for n, (which, first) in enumerate(BLOCKS):
        target = (scale_gate, scale_up)[which]
        target[first : first + 2] = scale[
            2 * n % 8 : 2 * n % 8 + 2, n // 4 * COLS : n // 4 * COLS + COLS
        ]
    arrived_z(1, nm_z)
    along_y(5, lambda there: nm_z, nm_y)
    nm_y[y] = nm_z[...]
    arrived_z(2, rt_z)
    along_y(6, lambda there: rt_z, rt_y)
    rt_y[y] = rt_z[...]

    arrived_z(4, ag_z)
    along_y(7, lambda there: ag_z, ag_y)
    ag_y[y] = ag_z[...]
    send_chunk(4)

    arrived_y(7, ag_y)
    rows = []
    for a in range(CODED // 4, 4):
        along = []
        for q in range(8):
            block = None
            for r in range(4):
                tile = ag_y[r, q]
                moved = pltpu.roll(tile, (32 * (r - a)) % 128, 1) if a != r else tile
                block = moved if block is None else jnp.where(lane == r, moved, block)
            along.append(block)
        rows.append(along)

    for c in range(CODED, len(CHUNKS)):
        first, count = CHUNKS[c]
        for p in range(first, first + count):
            for q in range(8):
                g = 2 * p
                x = tile_of(
                    w[g : g + 2, :, 128 * q : 128 * q + 128],
                    rows[g // 8 - CODED // 4][q][g % 8 : g % 8 + 2],
                )
                tx[4 * q : 4 * q + 4, p] = x.T.astype(jnp.bfloat16).reshape(4, COLS, 128)
        send_chunk(c)

    back = ((1.0 / TOP) / scale).T
    back = jnp.concatenate([back[:COLS], back[COLS : 2 * COLS]], axis=1)
    arrived_y(5, nm_y)
    for k in range(PEERS):
        nm_t[k] = jnp.maximum(nm_y[k % 4, k // 4].astype(jnp.float32), LEAST).T
    mine = pl.ds(pl.multiple_of(COLS * y, COLS), COLS)
    for k in range(PEERS):
        turned[k] = nm_t[k, mine] * back

    arrived_y(6, rt_y)
    for k in range(PEERS // 2):
        low, high = joined(rt_y[2 * (k % 2), k // 2], rt_y[2 * (k % 2) + 1, k // 2])
        router_out[bank, :, 128 * k : 128 * k + 128] = jnp.concatenate([low, high], axis=0).astype(
            jnp.bfloat16
        )
    crossing = []
    half = lax.broadcasted_iota(jnp.int32, (COLS, 128), 1) < 64
    for hop in range(1, BANKS):
        copy = pltpu.make_async_remote_copy(
            src_ref=router_out.at[bank], dst_ref=router_out.at[bank],
            send_sem=x_send.at[hop - 1], recv_sem=x_recv.at[hop - 1],
            device_id={"bank": lax.rem(bank + hop, BANKS)}, device_id_type=MESH,
        )
        copy.start()
        crossing.append(copy)

    for c, (first, count) in enumerate(CHUNKS):
        bytes_of(rx.at[others, pl.ds(first, count)], recv.at[c])
        for p in range(first, first + count):
            for k in range(PEERS // 2):
                pair = []
                for n in (2 * k, 2 * k + 1):
                    tile = rx[n, p]
                    if p < CODED:
                        both = turned[n]
                        factor = jnp.where(
                            half, both[:, 2 * p : 2 * p + 1], both[:, 2 * p + 1 : 2 * p + 2]
                        )
                        tile = decoded(tile, factor)
                    pair.append(tile)
                even, odd = joined(*pair)
                here = slice(128 * k, 128 * k + 128)
                placed[2 * p, :, here] = even.astype(jnp.bfloat16)
                placed[2 * p + 1, :, here] = odd.astype(jnp.bfloat16)

    for copy in crossing:
        copy.wait()
    for n, sent in enumerate((rs_y, nm_z, rt_z, rs_z, ag_z, nm_y, rt_y, ag_y)):
        bytes_of(sent.at[pl.ds(0, sent.shape[0] - 1)], stage_send.at[n])
    for c, (first, count) in enumerate(CHUNKS):
        bytes_of(tx.at[others, pl.ds(first, count)], send.at[c])


def store_kernel(placed, scale_gate, scale_up, router, *out):
    gate_out, up_out, scale_gate_out, scale_up_out, router_out, sem = out
    moves = [(scale_gate, scale_gate_out), (scale_up, scale_up_out)]
    runs = []
    for n, (which, first) in enumerate(BLOCKS):
        if runs and runs[-1][0] == which and runs[-1][1] + runs[-1][3] == first:
            runs[-1][3] += 2
        else:
            runs.append([which, first, 2 * n, 2])
    for which, first, at, count in runs:
        target = (gate_out, up_out)[which]
        moves.append((placed.at[pl.ds(at, count)], target.at[pl.ds(first, count)]))
    moves.append((router, router_out))
    copies = [pltpu.make_async_copy(a, b, sem.at[n]) for n, (a, b) in enumerate(moves)]
    for copy in copies:
        copy.start()
    for copy in copies:
        copy.wait()


def local(w_gate, w_up, router_weight, router_gain):
    f32, bf16 = jnp.float32, jnp.bfloat16
    vmem, anywhere = pl.BlockSpec(memory_space=pltpu.VMEM), pl.BlockSpec(memory_space=pl.ANY)
    dma = pltpu.SemaphoreType.DMA
    given = (w_gate, w_up, router_weight.T, router_gain.reshape(1, -1))
    served = jax.ShapeDtypeStruct((16, COLS, D_MODEL), bf16)
    scale = jax.ShapeDtypeStruct((16, COLS), f32)
    router = jax.ShapeDtypeStruct((BANKS, 16, D_MODEL), bf16)
    arrived = pl.pallas_call(
        spread_kernel,
        out_shape=(jax.ShapeDtypeStruct((MATS, COLS, D_MODEL), bf16), scale, scale, router),
        in_specs=[anywhere] * 4,
        out_specs=(vmem,) * 4,
        scratch_shapes=[
            pltpu.VMEM((MATS, 64, 1024), f32),
            pltpu.VMEM((4, 8, 8, 128), f32),
            pltpu.VMEM((4, 8, 8, 128), f32),
            pltpu.VMEM((8, 8, 128), f32),
            pltpu.VMEM((8, 8, 128), f32),
            pltpu.VMEM((8, 16, 128), bf16),
            pltpu.VMEM((8, 16, 128), bf16),
            pltpu.VMEM((4, 8, 16, 128), bf16),
            pltpu.VMEM((PEERS, 128, 16), f32),
            pltpu.VMEM((8, 128), f32),
            pltpu.VMEM((8, 8, 128), f32),
            pltpu.VMEM((4, 8, 8, 128), f32),
            pltpu.VMEM((PEERS, COLS, 16), f32),
            pltpu.VMEM((PEERS, PAIRS, COLS, 128), bf16),
            pltpu.VMEM((PEERS, PAIRS, COLS, 128), bf16),
            pltpu.VMEM((16, 64), f32),
            pltpu.VMEM((1, 64), f32),
            pltpu.VMEM((8, 128), bf16),
            pltpu.VMEM((8, 8, 128), bf16),
            pltpu.VMEM((4, 8, 8, 128), bf16),
            dma((PAIRS + 2,)),
            dma((8,)),
            dma((8,)),
            dma((BANKS - 1,)),
            dma((BANKS - 1,)),
            dma((len(CHUNKS),)),
            dma((len(CHUNKS),)),
        ],
        compiler_params=pltpu.CompilerParams(
            collective_id=0, has_side_effects=True, vmem_limit_bytes=46 * 2**20
        ),
    )(*[pltpu.with_memory_space_constraint(a, pltpu.HBM) for a in given])
    serve_gate, serve_up, scale_gate, scale_up, router = pl.pallas_call(
        store_kernel,
        out_shape=(served, served, scale, scale, router),
        in_specs=[vmem] * 4,
        out_specs=(anywhere,) * 5,
        scratch_shapes=[dma((16,))],
        compiler_params=pltpu.CompilerParams(vmem_limit_bytes=32 * 2**20),
    )(*arrived)
    return (
        jnp.swapaxes(serve_gate, 1, 2),
        jnp.swapaxes(serve_up, 1, 2),
        scale_gate,
        scale_up,
        router.reshape(BANKS * 16, D_MODEL).T,
    )


def solution(mesh):
    placed = (
        P(("trial", "bank"), "zero", None),
        P(("trial", "bank"), "zero", None),
        P(("trial", "zero"), "bank"),
        P(("trial", "zero")),
    )
    return jax.shard_map(
        local,
        mesh=mesh,
        in_specs=placed,
        out_specs=(
            P(("trial", "bank"), None, "zero"),
            P(("trial", "bank"), None, "zero"),
            P(("trial", "bank"), "zero"),
            P(("trial", "bank"), "zero"),
            P("trial", None),
        ),
        check_vma=False,
    )
```
